8 devices in a mesh: dp: 2 (over y, z), tp: 4 (over x, core).
Axes of the slice: x: 2, y: 2, z: 1, core: 2. Of those that a mesh axis runs over, the one named last changes fastest.
Arguments:
- x: bfloat16 [4096, 5120], P('dp'), parts along dimension 0
- w_gate: bfloat16 [5120, 17920], P(None, 'tp')
- w_up: bfloat16 [5120, 17920], P(None, 'tp')
- w_down: bfloat16 [17920, 5120], P('tp')
Outputs:
- output: bfloat16 [4096, 5120], P('dp'), parts along dimension 0
There are 2 independent parts. The reference program is written for one: setup_inputs(seed, part) draws one part's arguments, and reference() takes and returns one part's arrays. A program takes and returns all parts, laid end to end along the dimension named above; an argument that names none is the same for every part.
All inputs are finite; a program needn't handle non-finite values.
Results may differ from the reference program's by a relative error of at most 0.016.
Values are sent between devices in bfloat16 or wider.
A program may use at most 2 GiB of HBM per device.

```python
import jax
import jax.numpy as jnp

ROWS = 2048
D = 5120
FF = 17920


def setup_inputs(seed: int = 0, part: int = 0) -> dict:
    kx, kg, ku, kd = jax.random.split(jax.random.key(seed), 4)
    drawn = {
        "x": jax.random.normal(jax.random.fold_in(kx, part), (ROWS, D), jnp.float32),
        "w_gate": jax.random.normal(kg, (D, FF), jnp.float32) * D**-0.5,
        "w_up": jax.random.normal(ku, (D, FF), jnp.float32) * D**-0.5,
        "w_down": jax.random.normal(kd, (FF, D), jnp.float32) * FF**-0.5,
    }
    return {k: v.astype(jnp.bfloat16) for k, v in drawn.items()}


def reference(x, w_gate, w_up, w_down):
    gate = jnp.dot(x, w_gate, preferred_element_type=jnp.float32)
    up = jnp.dot(x, w_up, preferred_element_type=jnp.float32)
    hidden = (jax.nn.silu(gate) * up).astype(jnp.bfloat16)
    return jnp.dot(hidden, w_down, preferred_element_type=jnp.float32).astype(jnp.bfloat16)
```

```python
import jax
import jax.numpy as jnp
from jax import lax
from jax.experimental import pallas as pl
from jax.experimental.pallas import tpu as pltpu
from jax.sharding import PartitionSpec as P

BF = jnp.bfloat16
F32 = jnp.float32
CHUNK = 512
G = 640
T = 1280
Q = 640


def kernel(x, wg, wu, wd, y, xb, hb, wb, own, snd, rcv, csum, crcv, yb,
           xsem, wsem, psend, precv, csend, crecv, ylocal, ysend, yrecv, pfree, cfree):
    rows, depth = x.shape
    width = wg.shape[1]
    m, half = CHUNK, CHUNK // 2
    chunks, ng, nd, nq = rows // m, width // G, depth // T, depth // Q
    tp = lax.axis_index("tp")
    core = lax.rem(tp, 2)
    partner = tp + 1 - 2 * core
    peer = lax.rem(tp + 2, 4)

    def remote(src, dst, send, recv, to):
        return pltpu.make_async_remote_copy(
            src_ref=src, dst_ref=dst, send_sem=send, recv_sem=recv,
            device_id={"tp": to}, device_id_type=pl.DeviceIdType.MESH)

    def signal(sem, to):
        pl.semaphore_signal(sem, inc=1, device_id={"tp": to}, device_id_type=pl.DeviceIdType.MESH)

    def cols(i, size):
        return pl.ds(pl.multiple_of(i * size, 128), size)

    def rows_at(i, size):
        return pl.ds(pl.multiple_of(i, 16), size)

    def x_copies(ch):
        return [pltpu.make_async_copy(x.at[rows_at(ch * m + who * half, half), :],
                                      xb.at[pl.ds(k * half, half), :], xsem.at[k])
                for k, who in enumerate((1 - core, core))]

    def gu_copies(j, slot):
        return [pltpu.make_async_copy(w.at[:, cols(j, G)], wb.at[slot, :, pl.ds(k * G, G)], wsem.at[slot, k])
                for k, w in enumerate((wg, wu))]

    def d_copies(n, slot):
        return [pltpu.make_async_copy(wd.at[:, cols(n, T)], wb.at[slot, pl.ds(0, width), pl.ds(0, T)], wsem.at[slot, 0])]

    def start(copies):
        for c in copies:
            c.start()

    def wait(copies):
        for c in copies:
            c.wait()

    def term_copy(n):
        return remote(snd.at[n], rcv.at[n], psend.at[n], precv.at[n], partner)

    def sum_copy(q):
        return remote(csum.at[q], crcv.at[q], csend.at[q], crecv.at[q], peer)

    def y_copies(ch, q, s):
        there = y.at[rows_at(ch * m + core * half, half), cols(q, Q)]
        return (pltpu.make_async_copy(yb.at[s], there, ylocal.at[s]),
                remote(yb.at[s], there, ysend.at[s], yrecv.at[ch * nq + q], partner))

    def chip_sum(ch, n):
        term_copy(n).wait()
        s = own[lax.rem(n, 2)] + rcv[n].astype(F32)
        for k in range(T // Q):
            csum[n * (T // Q) + k] = s[:, k * Q:(k + 1) * Q].astype(BF)

        @pl.when(ch < chunks - 1)
        def _():
            signal(pfree, partner)

        @pl.when(ch > 0)
        def _():
            pl.semaphore_wait(cfree, T // Q)
        for k in range(T // Q):
            sum_copy(n * (T // Q) + k).start()

    def finish(ch, q):
        sum_copy(q).wait()
        s = lax.rem(q, 2)

        @pl.when(ch * nq + q >= 2)
        def _():
            here, there = y_copies(ch, q, s)
            here.wait()
            there.wait_send()
        yb[s] = (csum[q].astype(F32) + crcv[q].astype(F32)).astype(BF)
        for c in y_copies(ch, q, s):
            c.start()

        @pl.when(ch < chunks - 1)
        def _():
            signal(cfree, peer)

    start(x_copies(0))
    start(gu_copies(0, 0))
    barrier = pltpu.get_barrier_semaphore()
    signal(barrier, partner)
    signal(barrier, peer)
    pl.semaphore_wait(barrier, 2)

    def chunk(ch, _):
        base = ch * (ng + nd)
        wait(x_copies(ch))

        def gate_up(j, _):
            slot = lax.rem(base + j, 2)
            wait(gu_copies(j, slot))

            @pl.when(j < ng - 1)
            def _():
                start(gu_copies(j + 1, 1 - slot))

            @pl.when(j == ng - 1)
            def _():
                start(d_copies(0, 1 - slot))

            def unit(lo, size):
                w = jnp.concatenate([wb[slot, :, lo:lo + size], wb[slot, :, G + lo:G + lo + size]], axis=1)
                acc = jnp.dot(xb[...], w, preferred_element_type=F32)
                hb[:, pl.ds(pl.multiple_of(j * G + lo, 128), size)] = (
                    jax.nn.silu(acc[:, :size]) * acc[:, size:]).astype(BF)

            unit(0, 384)

            @pl.when((ch > 0) & (j == 0))
            def _():
                chip_sum(ch - 1, nd - 1)

            @pl.when(ch > 0)
            def _():
                finish(ch - 1, j)
            unit(384, 256)
            return 0

        lax.fori_loop(0, ng, gate_up, 0)

        @pl.when(ch < chunks - 1)
        def _():
            start(x_copies(ch + 1))

        def down(n, _):
            slot = lax.rem(base + ng + n, 2)
            wait(d_copies(n, slot))

            @pl.when(n < nd - 1)
            def _():
                start(d_copies(n + 1, 1 - slot))

            @pl.when((n == nd - 1) & (ch < chunks - 1))
            def _():
                start(gu_copies(0, 1 - slot))

            def unit(lo, size):
                acc = jnp.dot(hb[...], wb[slot, :width, lo:lo + size], preferred_element_type=F32)
                snd[n, :, lo:lo + size] = acc[:half].astype(BF)
                own[lax.rem(n, 2), :, lo:lo + size] = acc[half:]

            unit(0, 768)

            @pl.when(n > 0)
            def _():
                chip_sum(ch, n - 1)

            @pl.when((n == 0) & (ch > 0))
            def _():
                finish(ch - 1, nq - 1)
            unit(768, 512)

            @pl.when(ch > 0)
            def _():
                pl.semaphore_wait(pfree, 1)
            term_copy(n).start()
            return 0

        lax.fori_loop(0, nd, down, 0)
        return 0

    lax.fori_loop(0, chunks, chunk, 0)
    chip_sum(chunks - 1, nd - 1)

    def drain(q, _):
        finish(chunks - 1, q)
        return 0

    lax.fori_loop(0, nq, drain, 0)
    for s in range(2):
        here, there = y_copies(0, 0, s)
        here.wait()
        there.wait_send()

    def arrive(i, _):
        there = y.at[rows_at(0, half), pl.ds(0, Q)]
        remote(yb.at[0], there, ysend.at[0], yrecv.at[i], partner).wait_recv()
        return 0

    lax.fori_loop(0, chunks * nq, arrive, 0)


def solution(mesh):
    def step(x, w_gate, w_up, w_down):
        rows, depth = x.shape
        width = w_gate.shape[1]
        half, nd, nq = CHUNK // 2, depth // T, depth // Q
        dma = pltpu.SemaphoreType.DMA
        return pl.pallas_call(
            kernel,
            out_shape=jax.ShapeDtypeStruct((rows, depth), BF),
            in_specs=[pl.BlockSpec(memory_space=pl.ANY)] * 4,
            out_specs=pl.BlockSpec(memory_space=pl.ANY),
            scratch_shapes=[
                pltpu.VMEM((CHUNK, depth), BF),
                pltpu.VMEM((CHUNK, width), BF),
                pltpu.VMEM((2, depth, T), BF),
                pltpu.VMEM((2, half, T), F32),
                pltpu.VMEM((nd, half, T), BF),
                pltpu.VMEM((nd, half, T), BF),
                pltpu.VMEM((nq, half, Q), BF),
                pltpu.VMEM((nq, half, Q), BF),
                pltpu.VMEM((2, half, Q), BF),
                dma((2,)), dma((2, 2)),
                dma((nd,)), dma((nd,)),
                dma((nq,)), dma((nq,)),
                dma((2,)), dma((2,)), dma((rows // CHUNK * nq,)),
                pltpu.SemaphoreType.REGULAR,
                pltpu.SemaphoreType.REGULAR,
            ],
            compiler_params=pltpu.CompilerParams(
                collective_id=0, has_side_effects=True, vmem_limit_bytes=67043328),
            name="mlp",
        )(x, w_gate, w_up, w_down)

    return jax.shard_map(
        step,
        mesh=mesh,
        in_specs=(P("dp", None), P(None, "tp"), P(None, "tp"), P("tp", None)),
        out_specs=P("dp", None),
        check_vma=False,
    )
```

```python
import jax
import jax.numpy as jnp
from jax import lax
from jax.experimental import pallas as pl
from jax.experimental.pallas import tpu as pltpu
from jax.sharding import PartitionSpec as P

BF = jnp.bfloat16
F32 = jnp.float32
M0 = 544
G = 640
T = 1280
Q = 640
GPARTS = ((0, 384), (384, 256))
TPARTS = ((0, 768), (768, 512))
QPARTS = ((0, 640), (640, 640))


def kernel(x, wg, wu, wd, y, xb, hb, wb, own, snd, rcv, csum, crcv, yb,
           xsem, wsem, psend, precv, csend, crecv, ylocal, ysend, yrecv, pfree, cfree):
    rows, depth = x.shape
    width = wg.shape[1]
    ng, nd = width // G, depth // T
    nq = 2 * nd
    last = (rows - 1) // M0
    m1 = rows - last * M0
    tp = lax.axis_index("tp")
    core = lax.rem(tp, 2)
    partner = tp + 1 - 2 * core
    peer = lax.rem(tp + 2, 4)

    def remote(src, dst, send, recv, to):
        return pltpu.make_async_remote_copy(
            src_ref=src, dst_ref=dst, send_sem=send, recv_sem=recv,
            device_id={"tp": to}, device_id_type=pl.DeviceIdType.MESH)

    def signal(sem, to):
        pl.semaphore_signal(sem, inc=1, device_id={"tp": to}, device_id_type=pl.DeviceIdType.MESH)

    def at(i, size, tile=128):
        return pl.ds(pl.multiple_of(i, tile), size)

    def x_copies(ch, m):
        h = m // 2
        return [pltpu.make_async_copy(x.at[at(ch * M0 + who * h, h, 16), :],
                                      xb.at[pl.ds(k * h, h), :], xsem.at[k])
                for k, who in enumerate((1 - core, core))]

    def gu_copies(j, slot, part):
        lo, size = GPARTS[part]
        return [pltpu.make_async_copy(w.at[:, at(j * G + lo, size)],
                                      wb.at[slot, :, pl.ds(2 * lo + k * size, size)], wsem.at[slot, part, k])
                for k, w in enumerate((wg, wu))]

    def d_copies(n, slot, part):
        lo, size = TPARTS[part]
        return [pltpu.make_async_copy(wd.at[:, at(n * T + lo, size)],
                                      wb.at[slot, pl.ds(0, width), pl.ds(lo, size)], wsem.at[slot, part, 0])]

    def start(copies):
        for c in copies:
            c.start()

    def wait(copies):
        for c in copies:
            c.wait()

    def term_copy(n, part, h):
        lo, size = TPARTS[part]
        there = (n, pl.ds(0, h), pl.ds(lo, size))
        return remote(snd.at[there], rcv.at[there], psend.at[2 * n + part], precv.at[2 * n + part], partner)

    def sum_copy(n, part, h, parts):
        lo, size = parts[part]
        there = (n, pl.ds(0, h), pl.ds(lo, size))
        return remote(csum.at[there], crcv.at[there], csend.at[2 * n + part], crecv.at[2 * n + part], peer)

    def y_copies(ch, n, part, h, parts):
        lo, size = parts[part]
        s = part
        here = yb.at[s, pl.ds(0, h), pl.ds(0, size)]
        there = y.at[at(ch * M0 + core * h, h, 16), at(n * T + lo, size)]
        return (pltpu.make_async_copy(here, there, ylocal.at[s]),
                remote(here, there, ysend.at[s], yrecv.at[ch * nq + 2 * n + part], partner))

    def y_free(part, h, parts):
        here, there = y_copies(0, 0, part, h, parts)
        here.wait()
        there.wait_send()

    def send_term(n, part, h, first):
        if first is False:
            pl.semaphore_wait(pfree, 1)
        elif first is not True:
            @pl.when(first == 0)
            def _():
                pl.semaphore_wait(pfree, 1)
        term_copy(n, part, h).start()

    def add_chip(n, part, h):
        lo, size = TPARTS[part]
        csum[n, :h, lo:lo + size] = (
            own[lax.rem(n, 2), :h, lo:lo + size] + rcv[n, :h, lo:lo + size].astype(F32)).astype(BF)

    def add_final(n, part, h, parts, cols):
        lo, size = parts[part]
        if cols is None:
            a, b = csum[n, :h, lo:lo + size], crcv[n, :h, lo:lo + size]
        else:
            a, b = csum[n, :h, cols], crcv[n, :h, cols]
        yb[part, :h, :size] = (a.astype(F32) + b.astype(F32)).astype(BF)

    def gate_up(ch, m, hp):
        base = ch * (ng + nd)
        wait(x_copies(ch, m))

        def tile(j, _):
            slot = lax.rem(base + j, 2)
            wait(gu_copies(j, slot, 0))
            if hp:
                wait(gu_copies(j, slot, 1))
            for part in (0, 1):
                @pl.when(j < ng - 1)
                def _():
                    start(gu_copies(j + 1, 1 - slot, part))

                @pl.when(j == ng - 1)
                def _():
                    start(d_copies(0, 1 - slot, part))
            if hp:
                n, part = lax.div(j, 2), lax.rem(j, 2)
                lo = pl.multiple_of(part * Q, 128)
                q = 2 * n + part

                @pl.when(j == 0)
                def _():
                    for p in (0, 1):
                        term_copy(nd - 1, p, hp).wait()
                        add_chip(nd - 1, p, hp)
                        signal(pfree, partner)

                    @pl.when(ch > 1)
                    def _():
                        pl.semaphore_wait(cfree, 2)
                    for p in (0, 1):
                        sum_copy(nd - 1, p, hp, QPARTS).start()
                there = (n, pl.ds(0, hp), pl.ds(lo, Q))
                remote(csum.at[there], crcv.at[there], csend.at[q], crecv.at[q], peer).wait()
                here = yb.at[part, pl.ds(0, hp), pl.ds(0, Q)]
                out = y.at[at((ch - 1) * M0 + core * hp, hp, 16), at(j * Q, Q)]
                copies = (pltpu.make_async_copy(here, out, ylocal.at[part]),
                          remote(here, out, ysend.at[part], yrecv.at[(ch - 1) * nq + j], partner))

                @pl.when((ch > 1) | (j > 1))
                def _():
                    copies[0].wait()
                    copies[1].wait_send()

            def unit(p):
                lo, size = GPARTS[p]
                acc = jnp.dot(xb[:m], wb[slot, :, 2 * lo:2 * (lo + size)], preferred_element_type=F32)
                hb[:m, at(j * G + lo, size)] = (jax.nn.silu(acc[:, :size]) * acc[:, size:]).astype(BF)

            unit(0)
            if hp:
                yb[part, :hp, :Q] = (csum[n, :hp, pl.ds(lo, Q)].astype(F32)
                                     + crcv[n, :hp, pl.ds(lo, Q)].astype(F32)).astype(BF)
            else:
                wait(gu_copies(j, slot, 1))
            unit(1)
            if hp:
                start(copies)
                signal(cfree, peer)
            return 0

        lax.fori_loop(0, ng, tile, 0)

    def final_prev(ch, hp):
        sum_copy(nd - 1, 1, hp, QPARTS).wait()
        y_free(1, hp, QPARTS)
        add_final(nd - 1, 1, hp, QPARTS, None)
        start(y_copies(ch - 1, nd - 1, 1, hp, QPARTS))
        signal(cfree, peer)

    def down(ch, m, hp, end):
        base = ch * (ng + nd) + ng
        h = m // 2

        def tile(n, first_tile):
            slot = lax.rem(base + n, 2)
            for part in (0, 1):
                wait(d_copies(n, slot, part))

            @pl.when(n < nd - 1)
            def _():
                for part in (0, 1):
                    start(d_copies(n + 1, 1 - slot, part))
            if not end:
                for part in (0, 1):
                    @pl.when((n == nd - 1) & (ch < last))
                    def _():
                        start(gu_copies(0, 1 - slot, part))

            def unit(p):
                lo, size = TPARTS[p]
                acc = jnp.dot(hb[:m], wb[slot, :width, lo:lo + size], preferred_element_type=F32)
                snd[n, :h, lo:lo + size] = acc[:h].astype(BF)
                own[lax.rem(n, 2), :h, lo:lo + size] = acc[h:]

            first = False if end else (ch == 0).astype(jnp.int32)

            def credit(k):
                if end:
                    pl.semaphore_wait(cfree, k)
                else:
                    @pl.when(ch > 0)
                    def _():
                        pl.semaphore_wait(cfree, k)

            unit(0)
            send_term(n, 0, h, first)
            if first_tile:
                if end:
                    final_prev(ch, hp)
                else:
                    @pl.when(ch > 0)
                    def _():
                        final_prev(ch, hp)
            elif end:
                term_copy(n - 1, 1, h).wait()
                add_chip(n - 1, 1, h)
                sum_copy(n - 1, 1, h, TPARTS).start()
            else:
                for p in (0, 1):
                    term_copy(n - 1, p, h).wait()
                for p in (0, 1):
                    add_chip(n - 1, p, h)
            unit(1)
            send_term(n, 1, h, first)
            if end:
                term_copy(n, 0, h).wait()
                add_chip(n, 0, h)
                credit(2)
                sum_copy(n, 0, h, TPARTS).start()
            elif not first_tile:
                for _ in (0, 1):
                    signal(pfree, partner)
                credit(2)
                for p in (0, 1):
                    sum_copy(n - 1, p, h, QPARTS).start()

        def loop(n, _):
            tile(n, False)
            return 0

        tile(0, True)
        lax.fori_loop(1, nd, loop, 0)

    h0, h1 = M0 // 2, m1 // 2
    start(x_copies(0, M0))
    for part in (0, 1):
        start(gu_copies(0, 0, part))
    barrier = pltpu.get_barrier_semaphore()
    signal(barrier, partner)
    signal(barrier, peer)
    pl.semaphore_wait(barrier, 2)

    gate_up(0, M0, None)

    def chunk(ch, _):
        @pl.when(ch < last - 1)
        def _():
            start(x_copies(ch + 1, M0))

        @pl.when(ch == last - 1)
        def _():
            start(x_copies(last, m1))
        down(ch, M0, h0, False)

        @pl.when(ch < last - 1)
        def _():
            gate_up(ch + 1, M0, h0)

        @pl.when(ch == last - 1)
        def _():
            gate_up(ch + 1, m1, h0)
        return 0

    lax.fori_loop(0, last, chunk, 0)
    down(last, m1, h0, True)
    term_copy(nd - 1, 1, h1).wait()
    add_chip(nd - 1, 1, h1)
    sum_copy(nd - 1, 1, h1, TPARTS).start()
    for n in range(nd):
        for part in (0, 1):
            sum_copy(n, part, h1, TPARTS).wait()
            if n == 0:
                y_free(part, h0, QPARTS)
            else:
                y_free(part, h1, TPARTS)
            add_final(n, part, h1, TPARTS, None)
            start(y_copies(last, n, part, h1, TPARTS))
    for part in (0, 1):
        y_free(part, h1, TPARTS)

    def arrive(i, _):
        there = y.at[pl.ds(0, h0), pl.ds(0, Q)]
        remote(yb.at[0, pl.ds(0, h0), pl.ds(0, Q)], there, ysend.at[0], yrecv.at[i], partner).wait_recv()
        return 0

    lax.fori_loop(0, last * nq, arrive, 0)
    for n in range(nd):
        for part in (0, 1):
            y_copies(last, n, part, h1, TPARTS)[1].wait_recv()


def solution(mesh):
    def step(x, w_gate, w_up, w_down):
        rows, depth = x.shape
        width = w_gate.shape[1]
        half, nd = M0 // 2, depth // T
        dma = pltpu.SemaphoreType.DMA
        return pl.pallas_call(
            kernel,
            out_shape=jax.ShapeDtypeStruct((rows, depth), BF),
            in_specs=[pl.BlockSpec(memory_space=pl.ANY)] * 4,
            out_specs=pl.BlockSpec(memory_space=pl.ANY),
            scratch_shapes=[
                pltpu.VMEM((M0, depth), BF),
                pltpu.VMEM((M0, width), BF),
                pltpu.VMEM((2, depth, T), BF),
                pltpu.VMEM((2, half, T), F32),
                pltpu.VMEM((nd, half, T), BF),
                pltpu.VMEM((nd, half, T), BF),
                pltpu.VMEM((nd, half, T), BF),
                pltpu.VMEM((nd, half, T), BF),
                pltpu.VMEM((2, half, TPARTS[0][1]), BF),
                dma((2,)), dma((2, 2, 2)),
                dma((2 * nd,)), dma((2 * nd,)),
                dma((2 * nd,)), dma((2 * nd,)),
                dma((2,)), dma((2,)), dma((-(-rows // M0) * 2 * nd,)),
                pltpu.SemaphoreType.REGULAR,
                pltpu.SemaphoreType.REGULAR,
            ],
            compiler_params=pltpu.CompilerParams(
                collective_id=0, has_side_effects=True, vmem_limit_bytes=67043328),
            name="mlp",
        )(x, w_gate, w_up, w_down)

    return jax.shard_map(
        step,
        mesh=mesh,
        in_specs=(P("dp", None), P(None, "tp"), P(None, "tp"), P("tp", None)),
        out_specs=P("dp", None),
        check_vma=False,
    )
```

```python
import jax
import jax.numpy as jnp
from jax import lax
from jax.experimental import pallas as pl
from jax.experimental.pallas import tpu as pltpu
from jax.sharding import PartitionSpec as P

BF = jnp.bfloat16
F32 = jnp.float32
M0 = 576
G = 640
T = 1280
Q = 640
GPARTS = ((0, 384), (384, 256))
TPARTS = ((0, 768), (768, 512))
QPARTS = ((0, 640), (640, 640))


def kernel(x, wg, wu, wd, y, wb, xb, hb, own, snd, rcv, csum, crcv, yb,
           xsem, wsem, psend, precv, csend, crecv, ylocal, ysend, yrecv, vsem, pfree, cfree, vfree):
    rows, depth = x.shape
    width = wg.shape[1]
    ng, nd = width // G, depth // T
    nq = 2 * nd
    last = (rows - 1) // M0
    m1 = rows - last * M0
    tp = lax.axis_index("tp")
    core = lax.rem(tp, 2)
    partner = tp + 1 - 2 * core
    peer = lax.rem(tp + 2, 4)

    def remote(src, dst, send, recv, to):
        return pltpu.make_async_remote_copy(
            src_ref=src, dst_ref=dst, send_sem=send, recv_sem=recv,
            device_id={"tp": to}, device_id_type=pl.DeviceIdType.MESH)

    def signal(sem, to):
        pl.semaphore_signal(sem, inc=1, device_id={"tp": to}, device_id_type=pl.DeviceIdType.MESH)

    def at(i, size, tile=128):
        return pl.ds(pl.multiple_of(i, tile), size)

    def x_copies(ch, m):
        h = m // 2
        return [pltpu.make_async_copy(x.at[at(ch * M0 + who * h, h, 16), :],
                                      xb.at[pl.ds(k * h, h), :], xsem.at[k])
                for k, who in enumerate((1 - core, core))]

    def gu_copies(j, slot, part):
        lo, size = GPARTS[part]
        return [pltpu.make_async_copy(w.at[:, at(j * G + lo, size)],
                                      wb.at[slot, :, pl.ds(2 * lo + k * size, size)], wsem.at[slot, part, k])
                for k, w in enumerate((wg, wu))]

    def d_copies(n, slot, part):
        lo, size = TPARTS[part]
        return [pltpu.make_async_copy(wd.at[:, at(n * T + lo, size)],
                                      wb.at[slot, pl.ds(0, width), pl.ds(lo, size)], wsem.at[slot, part, 0])]

    def start(copies):
        for c in copies:
            c.start()

    def wait(copies):
        for c in copies:
            c.wait()

    def term_copy(n, part, h):
        lo, size = TPARTS[part]
        there = (n, pl.ds(0, h), pl.ds(lo, size))
        return remote(snd.at[there], rcv.at[there], psend.at[2 * n + part], precv.at[2 * n + part], partner)

    def sum_copy(n, part, h, parts):
        lo, size = parts[part]
        there = (n, pl.ds(0, h), pl.ds(lo, size))
        return remote(csum.at[there], crcv.at[there], csend.at[2 * n + part], crecv.at[2 * n + part], peer)

    def y_copies(ch, n, part, h, parts):
        lo, size = parts[part]
        s = part
        here = yb.at[s, pl.ds(0, h), pl.ds(0, size)]
        there = y.at[at(ch * M0 + core * h, h, 16), at(n * T + lo, size)]
        return (pltpu.make_async_copy(here, there, ylocal.at[s]),
                remote(here, there, ysend.at[s], yrecv.at[ch * nq + 2 * n + part], partner))

    def spot(n, row, size):
        return n // 2, at((n % 2) * rows + row, size, 16)

    def end_copy(n, part, h):
        lo, size = TPARTS[part]
        slot, there = spot(n, last * M0 + core * h, h)
        here = wb.at[slot, there, pl.ds(lo, size)]
        return remote(here, here, csend.at[2 * n + part], yrecv.at[last * nq + 2 * n + part], partner)

    def load_copies(n):
        slot, there = spot(n, 0, last * M0)
        return pltpu.make_async_copy(y.at[:, pl.ds(n * T, T)], wb.at[slot, there, :], vsem.at[n])

    def y_free(part, h, parts):
        here, there = y_copies(0, 0, part, h, parts)
        here.wait()
        there.wait_send()

    def send_term(n, part, h, first):
        if first is False:
            pl.semaphore_wait(pfree, 1)
        elif first is not True:
            @pl.when(first == 0)
            def _():
                pl.semaphore_wait(pfree, 1)
        term_copy(n, part, h).start()

    def add_chip(n, part, h):
        lo, size = TPARTS[part]
        csum[n, :h, lo:lo + size] = (
            own[lax.rem(n, 2), :h, lo:lo + size] + rcv[n, :h, lo:lo + size].astype(F32)).astype(BF)

    def add_final(n, part, h, parts, cols):
        lo, size = parts[part]
        if cols is None:
            a, b = csum[n, :h, lo:lo + size], crcv[n, :h, lo:lo + size]
        else:
            a, b = csum[n, :h, cols], crcv[n, :h, cols]
        yb[part, :h, :size] = (a.astype(F32) + b.astype(F32)).astype(BF)

    def gate_up(ch, m, hp, ahead):
        base = ch * (ng + nd)
        wait(x_copies(ch, m))
        split = ahead or not hp

        def tile(j, _):
            slot = lax.rem(base + j, 2)
            wait(gu_copies(j, slot, 0))
            if not split:
                wait(gu_copies(j, slot, 1))

            def fetch(tile_no, where, part):
                @pl.when(tile_no < ng)
                def _():
                    start(gu_copies(tile_no, where, part))

                @pl.when(tile_no >= ng)
                def _():
                    start(d_copies(tile_no - ng, where, part))

            if ahead:
                @pl.when(j == 0)
                def _():
                    for part in (0, 1):
                        start(gu_copies(1, 1 - slot, part))
            else:
                for part in (0, 1):
                    fetch(j + 1, 1 - slot, part)
            if hp:
                n, part = lax.div(j, 2), lax.rem(j, 2)
                lo = pl.multiple_of(part * Q, 128)
                q = 2 * n + part
                there = (n, pl.ds(0, hp), pl.ds(lo, Q))
                remote(csum.at[there], crcv.at[there], csend.at[q], crecv.at[q], peer).wait()
                here = yb.at[part, pl.ds(0, hp), pl.ds(0, Q)]
                out = y.at[at((ch - 1) * M0 + core * hp, hp, 16), at(j * Q, Q)]
                copies = (pltpu.make_async_copy(here, out, ylocal.at[part]),
                          remote(here, out, ysend.at[part], yrecv.at[(ch - 1) * nq + j], partner))

                @pl.when((ch > 1) | (j > 1))
                def _():
                    copies[0].wait()
                    copies[1].wait_send()

            def unit(p):
                lo, size = GPARTS[p]
                for k in range(0, size, 128):
                    w = jnp.concatenate([wb[slot, :, c:c + 128] for c in (2 * lo + k, 2 * lo + size + k)], axis=1)
                    acc = jnp.dot(xb[:m], w, preferred_element_type=F32)
                    hb[:m, at(j * G + lo + k, 128)] = (jax.nn.silu(acc[:, :128]) * acc[:, 128:]).astype(BF)

            unit(0)
            if ahead:
                fetch(j + 2, slot, 0)
            if hp:
                @pl.when(j == 0)
                def _():
                    for p in (0, 1):
                        term_copy(nd - 1, p, hp).wait()
                        add_chip(nd - 1, p, hp)

                    for _ in (0, 1):
                        signal(pfree, partner)

                    @pl.when(ch > 1)
                    def _():
                        pl.semaphore_wait(cfree, 2)
                    for p in (0, 1):
                        sum_copy(nd - 1, p, hp, QPARTS).start()
            if split:
                wait(gu_copies(j, slot, 1))
            if hp:
                yb[part, :hp, :Q] = (csum[n, :hp, pl.ds(lo, Q)].astype(F32)
                                     + crcv[n, :hp, pl.ds(lo, Q)].astype(F32)).astype(BF)
            unit(1)
            if ahead:
                fetch(j + 2, slot, 1)
            if hp:
                start(copies)
                signal(cfree, peer)
            return 0

        lax.fori_loop(0, ng, tile, 0)

    def final_prev(ch, hp):
        sum_copy(nd - 1, 1, hp, QPARTS).wait()
        y_free(1, hp, QPARTS)
        add_final(nd - 1, 1, hp, QPARTS, None)
        start(y_copies(ch - 1, nd - 1, 1, hp, QPARTS))
        signal(cfree, peer)

    def down(ch, m, hp, end):
        base = ch * (ng + nd) + ng
        h = m // 2

        def tile(n, first_tile):
            slot = lax.rem(base + n, 2)
            for part in (0, 1):
                wait(d_copies(n, slot, part))

            def fetch(tile_no, where, part):
                @pl.when(tile_no < nd)
                def _():
                    start(d_copies(tile_no, where, part))

                if not end:
                    @pl.when(tile_no >= nd)
                    def _():
                        start(gu_copies(tile_no - nd, where, part))

            if not end:
                for part in (0, 1):
                    fetch(n + 1, 1 - slot, part)

            def unit(p):
                lo, size = TPARTS[p]
                for c in range(lo, lo + size, 256):
                    acc = jnp.dot(hb[:m], wb[slot, :width, c:c + 256], preferred_element_type=F32)
                    snd[n, :h, c:c + 256] = acc[:h].astype(BF)
                    own[lax.rem(n, 2), :h, c:c + 256] = acc[h:]

            first = False if end else (ch == 0).astype(jnp.int32)

            def credit(k):
                if end:
                    pl.semaphore_wait(cfree, k)
                else:
                    @pl.when(ch > 0)
                    def _():
                        pl.semaphore_wait(cfree, k)

            unit(0)
            if end:
                fetch(n + 2, slot, 0)
                send_term(n, 0, h, first)
            if first_tile:
                if end:
                    final_prev(ch, hp)
                else:
                    @pl.when(ch > 0)
                    def _():
                        final_prev(ch, hp)
            elif end:
                term_copy(n - 1, 1, h).wait()
                add_chip(n - 1, 1, h)
                sum_copy(n - 1, 1, h, TPARTS).start()
            else:
                for p in (0, 1):
                    term_copy(n - 1, p, h).wait()
                for p in (0, 1):
                    add_chip(n - 1, p, h)
            unit(1)
            if end:
                fetch(n + 2, slot, 1)
                send_term(n, 1, h, first)
                term_copy(n, 0, h).wait()
                add_chip(n, 0, h)
                credit(2)
                sum_copy(n, 0, h, TPARTS).start()
            else:
                for p in (0, 1):
                    send_term(n, p, h, first)
                if not first_tile:
                    for _ in (0, 1):
                        signal(pfree, partner)
                    credit(2)
                    for p in (0, 1):
                        sum_copy(n - 1, p, h, QPARTS).start()

        def loop(n, _):
            tile(n, False)
            return 0

        tile(0, True)
        lax.fori_loop(1, nd, loop, 0)

    h0, h1 = M0 // 2, m1 // 2
    start(x_copies(0, M0))
    for part in (0, 1):
        start(gu_copies(0, 0, part))
    barrier = pltpu.get_barrier_semaphore()
    signal(barrier, partner)
    signal(barrier, peer)
    pl.semaphore_wait(barrier, 2)

    gate_up(0, M0, None, False)

    def chunk(ch, _):
        @pl.when(ch < last - 1)
        def _():
            start(x_copies(ch + 1, M0))

        @pl.when(ch == last - 1)
        def _():
            start(x_copies(last, m1))
        down(ch, M0, h0, False)

        @pl.when(ch < last - 1)
        def _():
            gate_up(ch + 1, M0, h0, False)

        @pl.when(ch == last - 1)
        def _():
            gate_up(ch + 1, m1, h0, True)
        return 0

    lax.fori_loop(0, last, chunk, 0)
    down(last, m1, h0, True)
    signal(vfree, partner)
    term_copy(nd - 1, 1, h1).wait()
    add_chip(nd - 1, 1, h1)
    sum_copy(nd - 1, 1, h1, TPARTS).start()
    for part in (0, 1):
        y_free(part, h0, QPARTS)

    def arrive(i, _):
        there = y.at[pl.ds(0, h0), pl.ds(0, Q)]
        remote(yb.at[0, pl.ds(0, h0), pl.ds(0, Q)], there, ysend.at[0], yrecv.at[i], partner).wait_recv()
        return 0

    lax.fori_loop(0, last * nq, arrive, 0)
    for n in range(nd):
        load_copies(n).start()
    pl.semaphore_wait(vfree, 1)
    for n in range(nd):
        for part in (0, 1):
            lo, size = TPARTS[part]
            sum_copy(n, part, h1, TPARTS).wait()
            slot, there = spot(n, last * M0 + core * h1, h1)
            wb[slot, there, lo:lo + size] = (csum[n, :h1, lo:lo + size].astype(F32)
                                             + crcv[n, :h1, lo:lo + size].astype(F32)).astype(BF)
            end_copy(n, part, h1).start()
    for n in range(nd):
        load_copies(n).wait()
        for part in (0, 1):
            end_copy(n, part, h1).wait()


def unload(v, y, sem):
    rows, depth = y.shape
    cuts = 2
    copies = []
    for n in range(depth // T):
        for k in range(cuts):
            r = rows // cuts
            src = v.at[n // 2, pl.ds((n % 2) * rows + k * r, r), :]
            copies.append(pltpu.make_async_copy(src, y.at[pl.ds(k * r, r), pl.ds(n * T, T)], sem.at[cuts * n + k]))
    for c in copies:
        c.start()
    for c in copies:
        c.wait()


def solution(mesh):
    def step(x, w_gate, w_up, w_down):
        rows, depth = x.shape
        width = w_gate.shape[1]
        half, nd = M0 // 2, depth // T
        dma = pltpu.SemaphoreType.DMA
        any_space, vmem = pl.BlockSpec(memory_space=pl.ANY), pl.BlockSpec(memory_space=pltpu.VMEM)
        last = (rows - 1) // M0
        _, held = pl.pallas_call(
            kernel,
            out_shape=(jax.ShapeDtypeStruct((last * M0, depth), BF), pltpu.VMEM((2, depth, T), BF)),
            in_specs=[any_space] * 4,
            out_specs=(any_space, vmem),
            scratch_shapes=[
                pltpu.VMEM((M0, depth), BF),
                pltpu.VMEM((M0, width), BF),
                pltpu.VMEM((2, half, T), F32),
                pltpu.VMEM((nd, half, T), BF),
                pltpu.VMEM((nd, half, T), BF),
                pltpu.VMEM((nd, half, T), BF),
                pltpu.VMEM((nd, half, T), BF),
                pltpu.VMEM((2, half, Q), BF),
                dma((2,)), dma((2, 2, 2)),
                dma((2 * nd,)), dma((2 * nd,)),
                dma((2 * nd,)), dma((2 * nd,)),
                dma((2,)), dma((2,)), dma(((last + 1) * 2 * nd,)), dma((nd,)),
                pltpu.SemaphoreType.REGULAR,
                pltpu.SemaphoreType.REGULAR,
                pltpu.SemaphoreType.REGULAR,
            ],
            compiler_params=pltpu.CompilerParams(
                collective_id=0, has_side_effects=True, vmem_limit_bytes=40000000),
            name="mlp",
        )(x, w_gate, w_up, w_down)
        held = pltpu.with_memory_space_constraint(held, pltpu.VMEM)
        return pl.pallas_call(
            unload,
            out_shape=jax.ShapeDtypeStruct((rows, depth), BF),
            in_specs=[vmem],
            out_specs=any_space,
            scratch_shapes=[dma((2 * nd,))],
            compiler_params=pltpu.CompilerParams(vmem_limit_bytes=4000000),
            name="unload",
        )(held)

    return jax.shard_map(
        step,
        mesh=mesh,
        in_specs=(P("dp", None), P(None, "tp"), P(None, "tp"), P("tp", None)),
        out_specs=P("dp", None),
        check_vma=False,
    )
```

```python
import jax
import jax.numpy as jnp
from jax import lax
from jax.experimental import pallas as pl
from jax.experimental.pallas import tpu as pltpu
from jax.sharding import PartitionSpec as P

BF = jnp.bfloat16
F32 = jnp.float32
M0 = 544
G = 640
T = 1280
Q = 640
GPARTS = ((0, 384), (384, 256))
TPARTS = ((0, 768), (768, 512))
QPARTS = ((0, 640), (640, 640))


def kernel(x, wg, wu, wd, y, wb, xb, hb, own, snd, rcv, csum, crcv, yb,
           xsem, wsem, psend, precv, csend, crecv, ylocal, ysend, yrecv, vsem, pfree, cfree, vfree):
    rows, depth = x.shape
    width = wg.shape[1]
    ng, nd = width // G, depth // T
    nq = 2 * nd
    last = (rows - 1) // M0
    m1 = rows - last * M0
    tp = lax.axis_index("tp")
    core = lax.rem(tp, 2)
    partner = tp + 1 - 2 * core
    peer = lax.rem(tp + 2, 4)

    def remote(src, dst, send, recv, to):
        return pltpu.make_async_remote_copy(
            src_ref=src, dst_ref=dst, send_sem=send, recv_sem=recv,
            device_id={"tp": to}, device_id_type=pl.DeviceIdType.MESH)

    def signal(sem, to):
        pl.semaphore_signal(sem, inc=1, device_id={"tp": to}, device_id_type=pl.DeviceIdType.MESH)

    def at(i, size, tile=128):
        return pl.ds(pl.multiple_of(i, tile), size)

    def x_copies(ch, m):
        h = m // 2
        return [pltpu.make_async_copy(x.at[at(ch * M0 + who * h, h, 16), :],
                                      xb.at[pl.ds(k * h, h), :], xsem.at[k])
                for k, who in enumerate((1 - core, core))]

    def gu_copies(j, slot, part):
        lo, size = GPARTS[part]
        return [pltpu.make_async_copy(w.at[:, at(j * G + lo, size)],
                                      wb.at[slot, :, pl.ds(2 * lo + k * size, size)], wsem.at[slot, part, k])
                for k, w in enumerate((wg, wu))]

    def d_copies(n, slot, part):
        lo, size = TPARTS[part]
        return [pltpu.make_async_copy(wd.at[:, at(n * T + lo, size)],
                                      wb.at[slot, pl.ds(0, width), pl.ds(lo, size)], wsem.at[slot, part, 0])]

    def start(copies):
        for c in copies:
            c.start()

    def wait(copies):
        for c in copies:
            c.wait()

    def term_copy(n, part, h):
        lo, size = TPARTS[part]
        there = (n, pl.ds(0, h), pl.ds(lo, size))
        return remote(snd.at[there], rcv.at[there], psend.at[2 * n + part], precv.at[2 * n + part], partner)

    def sum_copy(n, part, h, parts):
        lo, size = parts[part]
        there = (n, pl.ds(0, h), pl.ds(lo, size))
        return remote(csum.at[there], crcv.at[there], csend.at[2 * n + part], crecv.at[2 * n + part], peer)

    def y_copies(ch, n, part, h, parts):
        lo, size = parts[part]
        s = part
        here = yb.at[s, pl.ds(0, h), pl.ds(0, size)]
        there = y.at[at(ch * M0 + core * h, h, 16), at(n * T + lo, size)]
        return (pltpu.make_async_copy(here, there, ylocal.at[s]),
                remote(here, there, ysend.at[s], yrecv.at[ch * nq + 2 * n + part], partner))

    def spot(n, row, size):
        return n // 2, at((n % 2) * rows + row, size, 16)

    def end_copy(n, part, h):
        lo, size = TPARTS[part]
        slot, there = spot(n, last * M0 + core * h, h)
        here = wb.at[slot, there, pl.ds(lo, size)]
        return remote(here, here, csend.at[2 * n + part], yrecv.at[last * nq + 2 * n + part], partner)

    def load_copies(n):
        slot, there = spot(n, 0, last * M0)
        return pltpu.make_async_copy(y.at[:, pl.ds(n * T, T)], wb.at[slot, there, :], vsem.at[n])

    def y_free(part, h, parts):
        here, there = y_copies(0, 0, part, h, parts)
        here.wait()
        there.wait_send()

    def send_term(n, part, h, first):
        if first is False:
            pl.semaphore_wait(pfree, 1)
        elif first is not True:
            @pl.when(first == 0)
            def _():
                pl.semaphore_wait(pfree, 1)
        term_copy(n, part, h).start()

    def add_chip(n, part, h):
        lo, size = TPARTS[part]
        csum[n, :h, lo:lo + size] = (
            own[lax.rem(n, 2), :h, lo:lo + size] + rcv[n, :h, lo:lo + size].astype(F32)).astype(BF)

    def add_final(n, part, h, parts, cols):
        lo, size = parts[part]
        if cols is None:
            a, b = csum[n, :h, lo:lo + size], crcv[n, :h, lo:lo + size]
        else:
            a, b = csum[n, :h, cols], crcv[n, :h, cols]
        yb[part, :h, :size] = (a.astype(F32) + b.astype(F32)).astype(BF)

    def gate_up(ch, m, hp, late):
        base = ch * (ng + nd)
        wait(x_copies(ch, m))

        def tile(j, _):
            slot = lax.rem(base + j, 2)
            for part in (0, 1):
                wait(gu_copies(j, slot, part))

            def fetch(tile_no, where, part):
                @pl.when(tile_no < ng)
                def _():
                    start(gu_copies(tile_no, where, part))

                @pl.when(tile_no >= ng)
                def _():
                    start(d_copies(tile_no - ng, where, part))

            for part in (0, 1):
                fetch(j + 1, 1 - slot, part)
            if hp:
                n, part = lax.div(j, 2), lax.rem(j, 2)
                lo = pl.multiple_of(part * Q, 128)
                q = 2 * n + part
                there = (n, pl.ds(0, hp), pl.ds(lo, Q))
                here = yb.at[part, pl.ds(0, hp), pl.ds(0, Q)]
                out = y.at[at((ch - 1) * M0 + core * hp, hp, 16), at(j * Q, Q)]
                copies = (pltpu.make_async_copy(here, out, ylocal.at[part]),
                          remote(here, out, ysend.at[part], yrecv.at[(ch - 1) * nq + j], partner))

            def ready():
                remote(csum.at[there], crcv.at[there], csend.at[q], crecv.at[q], peer).wait()

                @pl.when((ch > 1) | (j > 1))
                def _():
                    copies[0].wait()
                    copies[1].wait_send()

            def add():
                yb[part, :hp, :Q] = (csum[n, :hp, pl.ds(lo, Q)].astype(F32)
                                     + crcv[n, :hp, pl.ds(lo, Q)].astype(F32)).astype(BF)

            def unit(p):
                lo, size = GPARTS[p]
                for k in range(0, size, 128):
                    w = jnp.concatenate([wb[slot, :, c:c + 128] for c in (2 * lo + k, 2 * lo + size + k)], axis=1)
                    acc = jnp.dot(xb[:m], w, preferred_element_type=F32)
                    hb[:m, at(j * G + lo + k, 128)] = (jax.nn.silu(acc[:, :128]) * acc[:, 128:]).astype(BF)

            if hp and not late:
                ready()
            unit(0)
            if hp and not late:
                add()
            unit(1)
            if hp:
                @pl.when(j == 0)
                def _():
                    for p in (0, 1):
                        term_copy(nd - 1, p, hp).wait()
                        add_chip(nd - 1, p, hp)

                    for _ in (0, 1):
                        signal(pfree, partner)

                    @pl.when(ch > 1)
                    def _():
                        pl.semaphore_wait(cfree, 2)
                    for p in (0, 1):
                        sum_copy(nd - 1, p, hp, QPARTS).start()
                if late:
                    ready()
                    add()
                start(copies)
                signal(cfree, peer)
            return 0

        lax.fori_loop(0, ng, tile, 0)

    def final_prev(ch, hp):
        sum_copy(nd - 1, 1, hp, QPARTS).wait()
        y_free(1, hp, QPARTS)
        add_final(nd - 1, 1, hp, QPARTS, None)
        start(y_copies(ch - 1, nd - 1, 1, hp, QPARTS))
        signal(cfree, peer)

    def down(ch, m, hp, end):
        base = ch * (ng + nd) + ng
        h = m // 2

        def tile(n, first_tile):
            slot = lax.rem(base + n, 2)
            for part in (0, 1):
                wait(d_copies(n, slot, part))

            def fetch(tile_no, where, part):
                @pl.when(tile_no < nd)
                def _():
                    start(d_copies(tile_no, where, part))

                if not end:
                    @pl.when(tile_no >= nd)
                    def _():
                        start(gu_copies(tile_no - nd, where, part))

            for part in (0, 1):
                fetch(n + 1, 1 - slot, part)

            def unit(p):
                lo, size = TPARTS[p]
                for c in range(lo, lo + size, 256):
                    acc = jnp.dot(hb[:m], wb[slot, :width, c:c + 256], preferred_element_type=F32)
                    snd[n, :h, c:c + 256] = acc[:h].astype(BF)
                    own[lax.rem(n, 2), :h, c:c + 256] = acc[h:]

            first = False if end else (ch == 0).astype(jnp.int32)

            def credit(k):
                if end:
                    pl.semaphore_wait(cfree, k)
                else:
                    @pl.when(ch > 0)
                    def _():
                        pl.semaphore_wait(cfree, k)

            unit(0)
            if end:
                send_term(n, 0, h, first)
            if first_tile:
                if not end:
                    @pl.when(ch > 0)
                    def _():
                        final_prev(ch, hp)
            elif end:
                term_copy(n - 1, 1, h).wait()
                add_chip(n - 1, 1, h)
                sum_copy(n - 1, 1, h, TPARTS).start()

                @pl.when(n == 1)
                def _():
                    final_prev(ch, hp)
            else:
                for p in (0, 1):
                    term_copy(n - 1, p, h).wait()
                for p in (0, 1):
                    add_chip(n - 1, p, h)
            unit(1)
            if end:
                send_term(n, 1, h, first)
                term_copy(n, 0, h).wait()
                add_chip(n, 0, h)
                credit(2)
                sum_copy(n, 0, h, TPARTS).start()
            else:
                for p in (0, 1):
                    send_term(n, p, h, first)
                if not first_tile:
                    for _ in (0, 1):
                        signal(pfree, partner)
                    credit(2)
                    for p in (0, 1):
                        sum_copy(n - 1, p, h, QPARTS).start()

        def loop(n, _):
            tile(n, False)
            return 0

        tile(0, True)
        lax.fori_loop(1, nd, loop, 0)

    h0, h1 = M0 // 2, m1 // 2
    start(x_copies(0, M0))
    for part in (0, 1):
        start(gu_copies(0, 0, part))
    barrier = pltpu.get_barrier_semaphore()
    signal(barrier, partner)
    signal(barrier, peer)
    pl.semaphore_wait(barrier, 2)

    gate_up(0, M0, None, False)

    def chunk(ch, _):
        @pl.when(ch < last - 1)
        def _():
            start(x_copies(ch + 1, M0))

        @pl.when(ch == last - 1)
        def _():
            start(x_copies(last, m1))
        down(ch, M0, h0, False)

        @pl.when(ch < last - 1)
        def _():
            gate_up(ch + 1, M0, h0, False)

        @pl.when(ch == last - 1)
        def _():
            gate_up(ch + 1, m1, h0, True)
        return 0

    lax.fori_loop(0, last, chunk, 0)
    down(last, m1, h0, True)
    signal(vfree, partner)
    term_copy(nd - 1, 1, h1).wait()
    add_chip(nd - 1, 1, h1)
    sum_copy(nd - 1, 1, h1, TPARTS).start()
    for part in (0, 1):
        y_free(part, h0, QPARTS)

    def arrive(i, _):
        there = y.at[pl.ds(0, h0), pl.ds(0, Q)]
        remote(yb.at[0, pl.ds(0, h0), pl.ds(0, Q)], there, ysend.at[0], yrecv.at[i], partner).wait_recv()
        return 0

    lax.fori_loop(0, last * nq, arrive, 0)
    for n in range(nd):
        load_copies(n).start()
    pl.semaphore_wait(vfree, 1)
    for n in range(nd):
        for part in (0, 1):
            lo, size = TPARTS[part]
            sum_copy(n, part, h1, TPARTS).wait()
            slot, there = spot(n, last * M0 + core * h1, h1)
            wb[slot, there, lo:lo + size] = (csum[n, :h1, lo:lo + size].astype(F32)
                                             + crcv[n, :h1, lo:lo + size].astype(F32)).astype(BF)
            end_copy(n, part, h1).start()
    for n in range(nd):
        load_copies(n).wait()
        for part in (0, 1):
            end_copy(n, part, h1).wait()


def unload(v, y, sem):
    rows, depth = y.shape
    cuts = 2
    copies = []
    for n in range(depth // T):
        for k in range(cuts):
            r = rows // cuts
            src = v.at[n // 2, pl.ds((n % 2) * rows + k * r, r), :]
            copies.append(pltpu.make_async_copy(src, y.at[pl.ds(k * r, r), pl.ds(n * T, T)], sem.at[cuts * n + k]))
    for c in copies:
        c.start()
    for c in copies:
        c.wait()


def solution(mesh):
    def step(x, w_gate, w_up, w_down):
        rows, depth = x.shape
        width = w_gate.shape[1]
        half, nd = M0 // 2, depth // T
        dma = pltpu.SemaphoreType.DMA
        any_space, vmem = pl.BlockSpec(memory_space=pl.ANY), pl.BlockSpec(memory_space=pltpu.VMEM)
        last = (rows - 1) // M0
        _, held = pl.pallas_call(
            kernel,
            out_shape=(jax.ShapeDtypeStruct((last * M0, depth), BF), pltpu.VMEM((2, depth, T), BF)),
            in_specs=[any_space] * 4,
            out_specs=(any_space, vmem),
            scratch_shapes=[
                pltpu.VMEM((M0, depth), BF),
                pltpu.VMEM((M0, width), BF),
                pltpu.VMEM((2, half, T), F32),
                pltpu.VMEM((nd, half, T), BF),
                pltpu.VMEM((nd, half, T), BF),
                pltpu.VMEM((nd, half, T), BF),
                pltpu.VMEM((nd, half, T), BF),
                pltpu.VMEM((2, half, Q), BF),
                dma((2,)), dma((2, 2, 2)),
                dma((2 * nd,)), dma((2 * nd,)),
                dma((2 * nd,)), dma((2 * nd,)),
                dma((2,)), dma((2,)), dma(((last + 1) * 2 * nd,)), dma((nd,)),
                pltpu.SemaphoreType.REGULAR,
                pltpu.SemaphoreType.REGULAR,
                pltpu.SemaphoreType.REGULAR,
            ],
            compiler_params=pltpu.CompilerParams(
                collective_id=0, has_side_effects=True, vmem_limit_bytes=40000000),
            name="mlp",
        )(x, w_gate, w_up, w_down)
        held = pltpu.with_memory_space_constraint(held, pltpu.VMEM)
        return pl.pallas_call(
            unload,
            out_shape=jax.ShapeDtypeStruct((rows, depth), BF),
            in_specs=[vmem],
            out_specs=any_space,
            scratch_shapes=[dma((2 * nd,))],
            compiler_params=pltpu.CompilerParams(vmem_limit_bytes=4000000),
            name="unload",
        )(held)

    return jax.shard_map(
        step,
        mesh=mesh,
        in_specs=(P("dp", None), P(None, "tp"), P(None, "tp"), P("tp", None)),
        out_specs=P("dp", None),
        check_vma=False,
    )
```

```python
import jax
import jax.numpy as jnp
from jax import lax
from jax.experimental import pallas as pl
from jax.experimental.pallas import tpu as pltpu
from jax.sharding import PartitionSpec as P

BF = jnp.bfloat16
F32 = jnp.float32
M0 = 512
G = 640
T = 1280
Q = 640
GPARTS = ((0, 384), (384, 256))
TPARTS = ((0, 768), (768, 512))
QPARTS = ((0, 640), (640, 640))


def kernel(x, wg, wu, wd, y, wb, xb, hb, own, snd, rcv, csum, crcv, yb,
           xsem, wsem, psend, precv, csend, crecv, ylocal, ysend, yrecv, vsem, pfree, cfree, vfree):
    rows, depth = x.shape
    width = wg.shape[1]
    ng, nd = width // G, depth // T
    nq = 2 * nd
    last = (rows - 1) // M0
    m1 = rows - last * M0
    tp = lax.axis_index("tp")
    core = lax.rem(tp, 2)
    partner = tp + 1 - 2 * core
    peer = lax.rem(tp + 2, 4)

    def remote(src, dst, send, recv, to):
        return pltpu.make_async_remote_copy(
            src_ref=src, dst_ref=dst, send_sem=send, recv_sem=recv,
            device_id={"tp": to}, device_id_type=pl.DeviceIdType.MESH)

    def signal(sem, to):
        pl.semaphore_signal(sem, inc=1, device_id={"tp": to}, device_id_type=pl.DeviceIdType.MESH)

    def at(i, size, tile=128):
        return pl.ds(pl.multiple_of(i, tile), size)

    def x_copies(ch, m):
        h = m // 2
        return [pltpu.make_async_copy(x.at[at(ch * M0 + who * h, h, 16), :],
                                      xb.at[pl.ds(k * h, h), :], xsem.at[k])
                for k, who in enumerate((1 - core, core))]

    def gu_copies(j, slot, part):
        lo, size = GPARTS[part]
        return [pltpu.make_async_copy(w.at[:, at(j * G + lo, size)],
                                      wb.at[slot, :, pl.ds(2 * lo + k * size, size)], wsem.at[slot, part, k])
                for k, w in enumerate((wg, wu))]

    def d_copies(n, slot, part):
        lo, size = TPARTS[part]
        return [pltpu.make_async_copy(wd.at[:, at(n * T + lo, size)],
                                      wb.at[slot, pl.ds(0, width), pl.ds(lo, size)], wsem.at[slot, part, 0])]

    def start(copies):
        for c in copies:
            c.start()

    def wait(copies):
        for c in copies:
            c.wait()

    def term_copy(n, part, h):
        lo, size = TPARTS[part]
        there = (n, pl.ds(0, h), pl.ds(lo, size))
        return remote(snd.at[there], rcv.at[there], psend.at[2 * n + part], precv.at[2 * n + part], partner)

    def sum_copy(n, part, h, parts):
        lo, size = parts[part]
        there = (n, pl.ds(0, h), pl.ds(lo, size))
        return remote(csum.at[there], crcv.at[there], csend.at[2 * n + part], crecv.at[2 * n + part], peer)

    def y_copies(ch, n, part, h, parts):
        lo, size = parts[part]
        s = part
        here = yb.at[s, pl.ds(0, h), pl.ds(0, size)]
        there = y.at[at(ch * M0 + core * h, h, 16), at(n * T + lo, size)]
        return (pltpu.make_async_copy(here, there, ylocal.at[s]),
                remote(here, there, ysend.at[s], yrecv.at[ch * nq + 2 * n + part], partner))

    def spot(n, row, size):
        return n // 2, at((n % 2) * rows + row, size, 16)

    def end_copy(n, part, h):
        lo, size = TPARTS[part]
        slot, there = spot(n, last * M0 + core * h, h)
        here = wb.at[slot, there, pl.ds(lo, size)]
        return remote(here, here, csend.at[2 * n + part], yrecv.at[last * nq + 2 * n + part], partner)

    def load_copies(n):
        slot, there = spot(n, 0, last * M0)
        return pltpu.make_async_copy(y.at[:, pl.ds(n * T, T)], wb.at[slot, there, :], vsem.at[n])

    def y_free(part, h, parts):
        here, there = y_copies(0, 0, part, h, parts)
        here.wait()
        there.wait_send()

    def send_term(n, part, h, first):
        if first is False:
            pl.semaphore_wait(pfree, 1)
        elif first is not True:
            @pl.when(first == 0)
            def _():
                pl.semaphore_wait(pfree, 1)
        term_copy(n, part, h).start()

    def add_chip(n, part, h):
        lo, size = TPARTS[part]
        csum[n, :h, lo:lo + size] = (
            own[lax.rem(n, 2), :h, lo:lo + size] + rcv[n, :h, lo:lo + size].astype(F32)).astype(BF)

    def add_final(n, part, h, parts, cols):
        lo, size = parts[part]
        if cols is None:
            a, b = csum[n, :h, lo:lo + size], crcv[n, :h, lo:lo + size]
        else:
            a, b = csum[n, :h, cols], crcv[n, :h, cols]
        yb[part, :h, :size] = (a.astype(F32) + b.astype(F32)).astype(BF)

    def gate_up(ch, m, hp, late):
        base = ch * (ng + nd)
        wait(x_copies(ch, m))

        def tile(j, _):
            slot = lax.rem(base + j, 2)
            for part in (0, 1):
                wait(gu_copies(j, slot, part))

            def fetch(tile_no, where, part):
                @pl.when(tile_no < ng)
                def _():
                    start(gu_copies(tile_no, where, part))

                @pl.when(tile_no >= ng)
                def _():
                    start(d_copies(tile_no - ng, where, part))

            for part in (0, 1):
                fetch(j + 1, 1 - slot, part)
            if hp:
                n, part = lax.div(j, 2), lax.rem(j, 2)
                lo = pl.multiple_of(part * Q, 128)
                q = 2 * n + part
                there = (n, pl.ds(0, hp), pl.ds(lo, Q))
                here = yb.at[part, pl.ds(0, hp), pl.ds(0, Q)]
                out = y.at[at((ch - 1) * M0 + core * hp, hp, 16), at(j * Q, Q)]
                copies = (pltpu.make_async_copy(here, out, ylocal.at[part]),
                          remote(here, out, ysend.at[part], yrecv.at[(ch - 1) * nq + j], partner))

            def ready():
                remote(csum.at[there], crcv.at[there], csend.at[q], crecv.at[q], peer).wait()

                @pl.when((ch > 1) | (j > 1))
                def _():
                    copies[0].wait()
                    copies[1].wait_send()

            def add():
                yb[part, :hp, :Q] = (csum[n, :hp, pl.ds(lo, Q)].astype(F32)
                                     + crcv[n, :hp, pl.ds(lo, Q)].astype(F32)).astype(BF)

            def unit(p):
                lo, size = GPARTS[p]
                for k in range(0, size, 128):
                    w = jnp.concatenate([wb[slot, :, c:c + 128] for c in (2 * lo + k, 2 * lo + size + k)], axis=1)
                    acc = jnp.dot(xb[:m], w, preferred_element_type=F32)
                    hb[:m, at(j * G + lo + k, 128)] = (jax.nn.silu(acc[:, :128]) * acc[:, 128:]).astype(BF)

            if hp and not late:
                ready()
            unit(0)
            if hp and not late:
                add()
            unit(1)
            if hp:
                @pl.when(j == 0)
                def _():
                    for p in (0, 1):
                        term_copy(nd - 1, p, hp).wait()
                        add_chip(nd - 1, p, hp)

                    for _ in (0, 1):
                        signal(pfree, partner)

                    @pl.when(ch > 1)
                    def _():
                        pl.semaphore_wait(cfree, 2)
                    for p in (0, 1):
                        sum_copy(nd - 1, p, hp, QPARTS).start()
                if late:
                    ready()
                    add()
                start(copies)
                signal(cfree, peer)
            return 0

        lax.fori_loop(0, ng, tile, 0)

    def final_prev(ch, hp):
        sum_copy(nd - 1, 1, hp, QPARTS).wait()
        y_free(1, hp, QPARTS)
        add_final(nd - 1, 1, hp, QPARTS, None)
        start(y_copies(ch - 1, nd - 1, 1, hp, QPARTS))
        signal(cfree, peer)

    def down(ch, m, hp, end):
        base = ch * (ng + nd) + ng
        h = m // 2

        def tile(n, first_tile):
            slot = lax.rem(base + n, 2)
            for part in (0, 1):
                wait(d_copies(n, slot, part))

            def fetch(tile_no, where, part):
                @pl.when(tile_no < nd)
                def _():
                    start(d_copies(tile_no, where, part))

                if not end:
                    @pl.when(tile_no >= nd)
                    def _():
                        start(gu_copies(tile_no - nd, where, part))

            for part in (0, 1):
                fetch(n + 1, 1 - slot, part)

            def unit(p):
                lo, size = TPARTS[p]
                for c in range(lo, lo + size, 256):
                    acc = jnp.dot(hb[:m], wb[slot, :width, c:c + 256], preferred_element_type=F32)
                    snd[n, :h, c:c + 256] = acc[:h].astype(BF)
                    own[lax.rem(n, 2), :h, c:c + 256] = acc[h:]

            first = False if end else (ch == 0).astype(jnp.int32)

            def credit(k):
                if end:
                    pl.semaphore_wait(cfree, k)
                else:
                    @pl.when(ch > 0)
                    def _():
                        pl.semaphore_wait(cfree, k)

            unit(0)
            if end:
                send_term(n, 0, h, first)
            if first_tile:
                if not end:
                    @pl.when(ch > 0)
                    def _():
                        final_prev(ch, hp)
            elif end:
                term_copy(n - 1, 1, h).wait()
                add_chip(n - 1, 1, h)
                sum_copy(n - 1, 1, h, TPARTS).start()

                @pl.when(n == 1)
                def _():
                    final_prev(ch, hp)
            else:
                for p in (0, 1):
                    term_copy(n - 1, p, h).wait()
                for p in (0, 1):
                    add_chip(n - 1, p, h)
            unit(1)
            if end:
                send_term(n, 1, h, first)
                term_copy(n, 0, h).wait()
                add_chip(n, 0, h)
                credit(2)
                sum_copy(n, 0, h, TPARTS).start()
            else:
                for p in (0, 1):
                    send_term(n, p, h, first)
                if not first_tile:
                    for _ in (0, 1):
                        signal(pfree, partner)
                    credit(2)
                    for p in (0, 1):
                        sum_copy(n - 1, p, h, QPARTS).start()

        def loop(n, _):
            tile(n, False)
            return 0

        tile(0, True)
        lax.fori_loop(1, nd, loop, 0)

    h0, h1 = M0 // 2, m1 // 2
    start(x_copies(0, M0))
    for part in (0, 1):
        start(gu_copies(0, 0, part))
    barrier = pltpu.get_barrier_semaphore()
    signal(barrier, partner)
    signal(barrier, peer)
    pl.semaphore_wait(barrier, 2)

    gate_up(0, M0, None, False)

    def chunk(ch, _):
        if m1 == M0:
            start(x_copies(ch + 1, M0))
        else:
            @pl.when(ch < last - 1)
            def _():
                start(x_copies(ch + 1, M0))

            @pl.when(ch == last - 1)
            def _():
                start(x_copies(last, m1))
        down(ch, M0, h0, False)

        if m1 == M0:
            gate_up(ch + 1, M0, h0, False)
        else:
            @pl.when(ch < last - 1)
            def _():
                gate_up(ch + 1, M0, h0, False)

            @pl.when(ch == last - 1)
            def _():
                gate_up(ch + 1, m1, h0, True)
        return 0

    lax.fori_loop(0, last, chunk, 0)
    down(last, m1, h0, True)
    signal(vfree, partner)
    term_copy(nd - 1, 1, h1).wait()
    add_chip(nd - 1, 1, h1)
    sum_copy(nd - 1, 1, h1, TPARTS).start()
    for part in (0, 1):
        y_free(part, h0, QPARTS)

    def arrive(i, _):
        there = y.at[pl.ds(0, h0), pl.ds(0, Q)]
        remote(yb.at[0, pl.ds(0, h0), pl.ds(0, Q)], there, ysend.at[0], yrecv.at[i], partner).wait_recv()
        return 0

    lax.fori_loop(0, last * nq, arrive, 0)
    for n in range(nd):
        load_copies(n).start()
    pl.semaphore_wait(vfree, 1)
    for n in range(nd):
        for part in (0, 1):
            lo, size = TPARTS[part]
            sum_copy(n, part, h1, TPARTS).wait()
            slot, there = spot(n, last * M0 + core * h1, h1)
            wb[slot, there, lo:lo + size] = (csum[n, :h1, lo:lo + size].astype(F32)
                                             + crcv[n, :h1, lo:lo + size].astype(F32)).astype(BF)
            end_copy(n, part, h1).start()
    for n in range(nd):
        load_copies(n).wait()
        for part in (0, 1):
            end_copy(n, part, h1).wait()


def unload(v, y, sem):
    rows, depth = y.shape
    cuts = 2
    copies = []
    for n in range(depth // T):
        for k in range(cuts):
            r = rows // cuts
            src = v.at[n // 2, pl.ds((n % 2) * rows + k * r, r), :]
            copies.append(pltpu.make_async_copy(src, y.at[pl.ds(k * r, r), pl.ds(n * T, T)], sem.at[cuts * n + k]))
    for c in copies:
        c.start()
    for c in copies:
        c.wait()


def solution(mesh):
    def step(x, w_gate, w_up, w_down):
        rows, depth = x.shape
        width = w_gate.shape[1]
        half, nd = M0 // 2, depth // T
        dma = pltpu.SemaphoreType.DMA
        any_space, vmem = pl.BlockSpec(memory_space=pl.ANY), pl.BlockSpec(memory_space=pltpu.VMEM)
        last = (rows - 1) // M0
        _, held = pl.pallas_call(
            kernel,
            out_shape=(jax.ShapeDtypeStruct((last * M0, depth), BF), pltpu.VMEM((2, depth, T), BF)),
            in_specs=[any_space] * 4,
            out_specs=(any_space, vmem),
            scratch_shapes=[
                pltpu.VMEM((M0, depth), BF),
                pltpu.VMEM((M0, width), BF),
                pltpu.VMEM((2, half, T), F32),
                pltpu.VMEM((nd, half, T), BF),
                pltpu.VMEM((nd, half, T), BF),
                pltpu.VMEM((nd, half, T), BF),
                pltpu.VMEM((nd, half, T), BF),
                pltpu.VMEM((2, half, Q), BF),
                dma((2,)), dma((2, 2, 2)),
                dma((2 * nd,)), dma((2 * nd,)),
                dma((2 * nd,)), dma((2 * nd,)),
                dma((2,)), dma((2,)), dma(((last + 1) * 2 * nd,)), dma((nd,)),
                pltpu.SemaphoreType.REGULAR,
                pltpu.SemaphoreType.REGULAR,
                pltpu.SemaphoreType.REGULAR,
            ],
            compiler_params=pltpu.CompilerParams(
                collective_id=0, has_side_effects=True, vmem_limit_bytes=40000000),
            name="mlp",
        )(x, w_gate, w_up, w_down)
        held = pltpu.with_memory_space_constraint(held, pltpu.VMEM)
        return pl.pallas_call(
            unload,
            out_shape=jax.ShapeDtypeStruct((rows, depth), BF),
            in_specs=[vmem],
            out_specs=any_space,
            scratch_shapes=[dma((2 * nd,))],
            compiler_params=pltpu.CompilerParams(vmem_limit_bytes=4000000),
            name="unload",
        )(held)

    return jax.shard_map(
        step,
        mesh=mesh,
        in_specs=(P("dp", None), P(None, "tp"), P(None, "tp"), P("tp", None)),
        out_specs=P("dp", None),
        check_vma=False,
    )
```

```python
import jax
import jax.numpy as jnp
from jax import lax
from jax.experimental import pallas as pl
from jax.experimental.pallas import tpu as pltpu
from jax.sharding import PartitionSpec as P

BF = jnp.bfloat16
F32 = jnp.float32
M0 = 544
G = 640
T = 1280
Q = 640
GPARTS = ((0, 384), (384, 256))
TPARTS = ((0, 768), (768, 512))
QPARTS = ((0, 640), (640, 640))


def kernel(x, wg, wu, wd, y, wb, xb, hb, own, snd, rcv, csum, crcv, yb,
           xsem, wsem, psend, precv, csend, crecv, ylocal, ysend, yrecv, vsem, pfree, cfree, vfree):
    rows, depth = x.shape
    width = wg.shape[1]
    ng, nd = width // G, depth // T
    nq = 2 * nd
    last = (rows - 1) // M0
    m1 = rows - last * M0
    tp = lax.axis_index("tp")
    core = lax.rem(tp, 2)
    partner = tp + 1 - 2 * core
    peer = lax.rem(tp + 2, 4)

    def remote(src, dst, send, recv, to):
        return pltpu.make_async_remote_copy(
            src_ref=src, dst_ref=dst, send_sem=send, recv_sem=recv,
            device_id={"tp": to}, device_id_type=pl.DeviceIdType.MESH)

    def signal(sem, to):
        pl.semaphore_signal(sem, inc=1, device_id={"tp": to}, device_id_type=pl.DeviceIdType.MESH)

    def at(i, size, tile=128):
        return pl.ds(pl.multiple_of(i, tile), size)

    def x_copies(ch, m):
        h = m // 2
        return [pltpu.make_async_copy(x.at[at(ch * M0 + who * h, h, 16), :],
                                      xb.at[pl.ds(k * h, h), :], xsem.at[k])
                for k, who in enumerate((1 - core, core))]

    def gu_copies(j, slot, part):
        lo, size = GPARTS[part]
        return [pltpu.make_async_copy(w.at[:, at(j * G + lo, size)],
                                      wb.at[slot, :, pl.ds(2 * lo + k * size, size)], wsem.at[slot, part, k])
                for k, w in enumerate((wg, wu))]

    def d_copies(n, slot, part):
        lo, size = TPARTS[part]
        return [pltpu.make_async_copy(wd.at[:, at(n * T + lo, size)],
                                      wb.at[slot, pl.ds(0, width), pl.ds(lo, size)], wsem.at[slot, part, 0])]

    def start(copies):
        for c in copies:
            c.start()

    def wait(copies):
        for c in copies:
            c.wait()

    def term_copy(n, part, h):
        lo, size = TPARTS[part]
        there = (n, pl.ds(0, h), pl.ds(lo, size))
        return remote(snd.at[there], rcv.at[there], psend.at[2 * n + part], precv.at[2 * n + part], partner)

    def sum_copy(n, part, h, parts):
        lo, size = parts[part]
        there = (n, pl.ds(0, h), pl.ds(lo, size))
        return remote(csum.at[there], crcv.at[there], csend.at[2 * n + part], crecv.at[2 * n + part], peer)

    def y_copies(ch, n, part, h, parts):
        lo, size = parts[part]
        s = part
        here = yb.at[s, pl.ds(0, h), pl.ds(0, size)]
        there = y.at[at(ch * M0 + core * h, h, 16), at(n * T + lo, size)]
        return (pltpu.make_async_copy(here, there, ylocal.at[s]),
                remote(here, there, ysend.at[s], yrecv.at[ch * nq + 2 * n + part], partner))

    def spot(n, row, size):
        return n // 2, at((n % 2) * rows + row, size, 16)

    def end_copy(n, part, h):
        lo, size = TPARTS[part]
        slot, there = spot(n, last * M0 + core * h, h)
        here = wb.at[slot, there, pl.ds(lo, size)]
        return remote(here, here, csend.at[2 * n + part], yrecv.at[last * nq + 2 * n + part], partner)

    def load_copies(n):
        slot, there = spot(n, 0, last * M0)
        return pltpu.make_async_copy(y.at[:, pl.ds(n * T, T)], wb.at[slot, there, :], vsem.at[n])

    def y_free(part, h, parts):
        here, there = y_copies(0, 0, part, h, parts)
        here.wait()
        there.wait_send()

    def send_term(n, part, h, first):
        if first is False:
            pl.semaphore_wait(pfree, 1)
        elif first is not True:
            @pl.when(first == 0)
            def _():
                pl.semaphore_wait(pfree, 1)
        term_copy(n, part, h).start()

    def add_chip(n, part, h):
        lo, size = TPARTS[part]
        csum[n, :h, lo:lo + size] = (
            own[lax.rem(n, 2), :h, lo:lo + size] + rcv[n, :h, lo:lo + size].astype(F32)).astype(BF)

    def add_final(n, part, h, parts, cols):
        lo, size = parts[part]
        if cols is None:
            a, b = csum[n, :h, lo:lo + size], crcv[n, :h, lo:lo + size]
        else:
            a, b = csum[n, :h, cols], crcv[n, :h, cols]
        yb[part, :h, :size] = (a.astype(F32) + b.astype(F32)).astype(BF)

    def gate_up(ch, m, hp, late):
        base = ch * (ng + nd)
        wait(x_copies(ch, m))

        def tile(j, _):
            slot = lax.rem(base + j, 2)
            opening = isinstance(j, int)
            wait(gu_copies(j, slot, 0))
            (start if opening else wait)(gu_copies(j, slot, 1))

            def fetch(tile_no, where, part):
                @pl.when(tile_no < ng)
                def _():
                    start(gu_copies(tile_no, where, part))

                @pl.when(tile_no >= ng)
                def _():
                    start(d_copies(tile_no - ng, where, part))

            for part in (0, 1):
                fetch(j + 1, 1 - slot, part)
            if hp:
                n, part = lax.div(j, 2), lax.rem(j, 2)
                lo = pl.multiple_of(part * Q, 128)
                q = 2 * n + part
                there = (n, pl.ds(0, hp), pl.ds(lo, Q))
                here = yb.at[part, pl.ds(0, hp), pl.ds(0, Q)]
                out = y.at[at((ch - 1) * M0 + core * hp, hp, 16), at(j * Q, Q)]
                copies = (pltpu.make_async_copy(here, out, ylocal.at[part]),
                          remote(here, out, ysend.at[part], yrecv.at[(ch - 1) * nq + j], partner))

            def ready():
                remote(csum.at[there], crcv.at[there], csend.at[q], crecv.at[q], peer).wait()

                @pl.when((ch > 1) | (j > 1))
                def _():
                    copies[0].wait()
                    copies[1].wait_send()

            def add():
                yb[part, :hp, :Q] = (csum[n, :hp, pl.ds(lo, Q)].astype(F32)
                                     + crcv[n, :hp, pl.ds(lo, Q)].astype(F32)).astype(BF)

            def unit(p):
                lo, size = GPARTS[p]
                for k in range(0, size, 128):
                    w = jnp.concatenate([wb[slot, :, c:c + 128] for c in (2 * lo + k, 2 * lo + size + k)], axis=1)
                    acc = jnp.dot(xb[:m], w, preferred_element_type=F32)
                    hb[:m, at(j * G + lo + k, 128)] = (jax.nn.silu(acc[:, :128]) * acc[:, 128:]).astype(BF)

            if hp and not late:
                ready()
            unit(0)
            if hp and not late:
                add()
            if opening:
                wait(gu_copies(j, slot, 1))
            unit(1)
            if hp:
                @pl.when(j == 0)
                def _():
                    for p in (0, 1):
                        term_copy(nd - 1, p, hp).wait()
                        add_chip(nd - 1, p, hp)

                    for _ in (0, 1):
                        signal(pfree, partner)

                    @pl.when(ch > 1)
                    def _():
                        pl.semaphore_wait(cfree, 2)
                    for p in (0, 1):
                        sum_copy(nd - 1, p, hp, QPARTS).start()
                if late:
                    ready()
                    add()
                start(copies)
                signal(cfree, peer)
            return 0

        if not hp:
            tile(0, 0)
        lax.fori_loop(0 if hp else 1, ng, tile, 0)

    def final_prev(ch, hp):
        sum_copy(nd - 1, 1, hp, QPARTS).wait()
        y_free(1, hp, QPARTS)
        add_final(nd - 1, 1, hp, QPARTS, None)
        start(y_copies(ch - 1, nd - 1, 1, hp, QPARTS))
        signal(cfree, peer)

    def down(ch, m, hp, end):
        base = ch * (ng + nd) + ng
        h = m // 2

        def tile(n, first_tile):
            slot = lax.rem(base + n, 2)
            for part in (0, 1):
                wait(d_copies(n, slot, part))

            def fetch(tile_no, where, part):
                @pl.when(tile_no < nd)
                def _():
                    start(d_copies(tile_no, where, part))

                if not end:
                    @pl.when(tile_no >= nd)
                    def _():
                        start(gu_copies(tile_no - nd, where, part))

            for part in (0, 1):
                fetch(n + 1, 1 - slot, part)

            def unit(p):
                lo, size = TPARTS[p]
                for c in range(lo, lo + size, 256):
                    acc = jnp.dot(hb[:m], wb[slot, :width, c:c + 256], preferred_element_type=F32)
                    snd[n, :h, c:c + 256] = acc[:h].astype(BF)
                    own[lax.rem(n, 2), :h, c:c + 256] = acc[h:]

            first = False if end else (ch == 0).astype(jnp.int32)

            def credit(k):
                if end:
                    pl.semaphore_wait(cfree, k)
                else:
                    @pl.when(ch > 0)
                    def _():
                        pl.semaphore_wait(cfree, k)

            unit(0)
            if end:
                send_term(n, 0, h, first)
            if first_tile:
                if not end:
                    @pl.when(ch > 0)
                    def _():
                        final_prev(ch, hp)
            elif end:
                term_copy(n - 1, 1, h).wait()
                add_chip(n - 1, 1, h)
                sum_copy(n - 1, 1, h, TPARTS).start()

                @pl.when(n == 1)
                def _():
                    final_prev(ch, hp)
            else:
                for p in (0, 1):
                    term_copy(n - 1, p, h).wait()
                for p in (0, 1):
                    add_chip(n - 1, p, h)
            unit(1)
            if end:
                send_term(n, 1, h, first)
                term_copy(n, 0, h).wait()
                add_chip(n, 0, h)
                credit(2)
                sum_copy(n, 0, h, TPARTS).start()
            else:
                for p in (0, 1):
                    send_term(n, p, h, first)
                if not first_tile:
                    for _ in (0, 1):
                        signal(pfree, partner)
                    credit(2)
                    for p in (0, 1):
                        sum_copy(n - 1, p, h, QPARTS).start()

        def loop(n, _):
            tile(n, False)
            return 0

        tile(0, True)
        lax.fori_loop(1, nd, loop, 0)

    h0, h1 = M0 // 2, m1 // 2
    start(x_copies(0, M0))
    start(gu_copies(0, 0, 0))
    barrier = pltpu.get_barrier_semaphore()
    signal(barrier, partner)
    signal(barrier, peer)
    pl.semaphore_wait(barrier, 2)

    gate_up(0, M0, None, False)

    def chunk(ch, _):
        @pl.when(ch < last - 1)
        def _():
            start(x_copies(ch + 1, M0))

        @pl.when(ch == last - 1)
        def _():
            start(x_copies(last, m1))
        down(ch, M0, h0, False)

        @pl.when(ch < last - 1)
        def _():
            gate_up(ch + 1, M0, h0, False)

        @pl.when(ch == last - 1)
        def _():
            gate_up(ch + 1, m1, h0, True)
        return 0

    lax.fori_loop(0, last, chunk, 0)
    down(last, m1, h0, True)
    signal(vfree, partner)
    term_copy(nd - 1, 1, h1).wait()
    add_chip(nd - 1, 1, h1)
    sum_copy(nd - 1, 1, h1, TPARTS).start()
    for part in (0, 1):
        y_free(part, h0, QPARTS)

    def arrive(i, _):
        there = y.at[pl.ds(0, h0), pl.ds(0, Q)]
        remote(yb.at[0, pl.ds(0, h0), pl.ds(0, Q)], there, ysend.at[0], yrecv.at[i], partner).wait_recv()
        return 0

    lax.fori_loop(0, last * nq, arrive, 0)
    for n in range(nd):
        load_copies(n).start()
    pl.semaphore_wait(vfree, 1)
    for n in range(nd):
        for part in (0, 1):
            lo, size = TPARTS[part]
            sum_copy(n, part, h1, TPARTS).wait()
            slot, there = spot(n, last * M0 + core * h1, h1)
            wb[slot, there, lo:lo + size] = (csum[n, :h1, lo:lo + size].astype(F32)
                                             + crcv[n, :h1, lo:lo + size].astype(F32)).astype(BF)
            end_copy(n, part, h1).start()
    for n in range(nd):
        load_copies(n).wait()
        for part in (0, 1):
            end_copy(n, part, h1).wait()


def unload(v, y, sem):
    rows, depth = y.shape
    cuts = 2
    copies = []
    for n in range(depth // T):
        for k in range(cuts):
            r = rows // cuts
            src = v.at[n // 2, pl.ds((n % 2) * rows + k * r, r), :]
            copies.append(pltpu.make_async_copy(src, y.at[pl.ds(k * r, r), pl.ds(n * T, T)], sem.at[cuts * n + k]))
    for c in copies:
        c.start()
    for c in copies:
        c.wait()


def solution(mesh):
    def step(x, w_gate, w_up, w_down):
        rows, depth = x.shape
        width = w_gate.shape[1]
        half, nd = M0 // 2, depth // T
        dma = pltpu.SemaphoreType.DMA
        any_space, vmem = pl.BlockSpec(memory_space=pl.ANY), pl.BlockSpec(memory_space=pltpu.VMEM)
        last = (rows - 1) // M0
        _, held = pl.pallas_call(
            kernel,
            out_shape=(jax.ShapeDtypeStruct((last * M0, depth), BF), pltpu.VMEM((2, depth, T), BF)),
            in_specs=[any_space] * 4,
            out_specs=(any_space, vmem),
            scratch_shapes=[
                pltpu.VMEM((M0, depth), BF),
                pltpu.VMEM((M0, width), BF),
                pltpu.VMEM((2, half, T), F32),
                pltpu.VMEM((nd, half, T), BF),
                pltpu.VMEM((nd, half, T), BF),
                pltpu.VMEM((nd, half, T), BF),
                pltpu.VMEM((nd, half, T), BF),
                pltpu.VMEM((2, half, Q), BF),
                dma((2,)), dma((2, 2, 2)),
                dma((2 * nd,)), dma((2 * nd,)),
                dma((2 * nd,)), dma((2 * nd,)),
                dma((2,)), dma((2,)), dma(((last + 1) * 2 * nd,)), dma((nd,)),
                pltpu.SemaphoreType.REGULAR,
                pltpu.SemaphoreType.REGULAR,
                pltpu.SemaphoreType.REGULAR,
            ],
            compiler_params=pltpu.CompilerParams(
                collective_id=0, has_side_effects=True, vmem_limit_bytes=40000000),
            name="mlp",
        )(x, w_gate, w_up, w_down)
        held = pltpu.with_memory_space_constraint(held, pltpu.VMEM)
        return pl.pallas_call(
            unload,
            out_shape=jax.ShapeDtypeStruct((rows, depth), BF),
            in_specs=[vmem],
            out_specs=any_space,
            scratch_shapes=[dma((2 * nd,))],
            compiler_params=pltpu.CompilerParams(vmem_limit_bytes=4000000),
            name="unload",
        )(held)

    return jax.shard_map(
        step,
        mesh=mesh,
        in_specs=(P("dp", None), P(None, "tp"), P(None, "tp"), P("tp", None)),
        out_specs=P("dp", None),
        check_vma=False,
    )
```
